256 devices in a mesh: grp: 2 (over y), col: 32 (over z, core), blk: 4 (over x).
Axes of the slice: x: 4, y: 2, z: 16, core: 2. Of those that a mesh axis runs over, the one named last changes fastest.
The devices are a block of a 4x16x16 slice.
Arguments:
- boundary: bfloat16 [256, 192, 576], P(('grp', 'col'), 'blk'), parts along dimension 0, may hold values from -6 to 6
- row_tensor: bfloat16 [256, 6, 6, 6, 6], P(('grp', 'col')), parts along dimension 0, may hold values from -1.5 to 1.5
- left_proj: bfloat16 [256, 192, 576], P(('grp', 'col'), 'blk'), parts along dimension 0, may hold values from -0.75 to 0.75
- right_proj: bfloat16 [256, 192, 576], P(('grp', 'col'), 'blk'), parts along dimension 0, may hold values from -0.3125 to 0.3125
- leg_parity: int32 [256, 3, 6], P('grp'), parts along dimension 0, may hold values from 0 to 1
- bond_charges: int32 [256, 2], P('grp'), parts along dimension 0, may hold values from 32 to 96, as said below
Outputs:
- new_boundary: bfloat16 [256, 192, 576], P(('grp', 'col'), 'blk'), parts along dimension 0
The draws below stay inside these ranges and needn't reach their ends.
There are 2 independent parts, one for each index of `grp`. The reference program is written for one: setup_inputs(seed, part) draws one part's arguments, and reference() takes and returns one part's arrays. A program takes and returns all parts, laid end to end along the dimension named above; each array names one. Nothing has to cross between parts.
Inputs may be any that keep to these rules, and one draw needn't show every extreme that they name: `bond_charges`: odd counts are 128 minus these, so neither block of a bond holds more than 96 live rows; some bond has an even count of 96 and some bond an odd count of 96. `leg_parity`: [c, 0] is the horizontal leg left of column c, [c, 1] the vertical leg between boundary and row, [c, 2] the outgoing vertical leg.
All inputs are finite; a program needn't handle non-finite values.
Results may differ from the reference program's by a relative error of at most 0.0057.
Values may be sent and summed in bfloat16 or wider, within the bound.
No kernel may reach another device: no remote copies, remote signals or barrier semaphores. Data moves between devices by JAX's collectives and lax.ppermute only.
A program may use at most 64 MiB of HBM per device.

```python
import jax
import jax.numpy as jnp
from jax import lax

CHI = 128
BLOCK = 96
D = 6
COLS = 128
PAD = 192


def draw_bond_charges(key, part):
    first_key, second_key, third_key = jax.random.split(jax.random.fold_in(key, 17), 3)
    counts = jax.random.randint(first_key, (COLS, 2), CHI - BLOCK, BLOCK + 1, dtype=jnp.int32)
    even_full = jax.random.randint(second_key, (), 0, COLS, dtype=jnp.int32)
    odd_full = jax.random.randint(third_key, (), 0, COLS, dtype=jnp.int32)
    counts = counts.at[even_full, 0].set(BLOCK)
    counts = counts.at[odd_full, 1].set(CHI - BLOCK)
    return counts


def plant(drawn, stream_key, least, largest):
    spot = [jax.random.randint(jax.random.fold_in(stream_key, axis), (), 0, length) for axis, length in enumerate(drawn.shape)]
    longest = drawn.shape.index(max(drawn.shape))
    neighbour = spot[:longest] + [(spot[longest] + 1) % drawn.shape[longest]] + spot[longest + 1:]
    return drawn.at[tuple(spot)].set(least).at[tuple(neighbour)].set(largest)


def level_of(key, extent, cuts, least, top_value):
    def one(axis_at, parts):
        heights = jax.random.uniform(jax.random.fold_in(jax.random.fold_in(key, 6), axis_at), (parts,), jnp.float32, least / len(cuts), top_value / len(cuts))
        return jnp.repeat(jnp.exp(heights), extent[axis_at] // parts).reshape((-1,) + (1,) * (len(extent) - axis_at - 1))

    loudness = one(*cuts[0])
    for cut in cuts[1:]:
        loudness = loudness * one(*cut)
    return loudness


def bell_draw(key, shape, spread, reach, pieces=(), kind=jnp.bfloat16):
    drawn = spread * jax.random.normal(key, shape, jnp.float32)
    if pieces:
        drawn = drawn * level_of(key, shape, pieces, -0.22, 0.18)
    return jnp.clip(drawn, -reach, reach).astype(kind)


def setup_inputs(seed: int = 0, part: int = 0) -> dict:
    arg_keys = jax.random.split(jax.random.key(seed), 7)
    part_keys = jax.random.split(jax.random.fold_in(arg_keys[6], part), 7)
    return {
        "boundary": bell_draw(part_keys[0], (COLS, PAD, D * BLOCK), 1.0, 6.0, ((0, 32), (1, 4))),
        "row_tensor": bell_draw(part_keys[1], (COLS, D, D, D, D), (D * D // 2) ** -0.5, 1.5, ((0, 32),)),
        "left_proj": bell_draw(part_keys[2], (COLS, PAD, D * BLOCK), (CHI // 2) ** -0.5, 0.75, ((0, 32), (1, 4))),
        "right_proj": bell_draw(part_keys[3], (COLS, PAD, D * BLOCK), (D * CHI // 2) ** -0.5, 0.3125, ((0, 32), (1, 4))),
        "leg_parity": plant(jax.random.randint(part_keys[4], (COLS, 3, D), 0, 2), jax.random.fold_in(part_keys[4], 1), 0, 1).astype(jnp.int32),
        "bond_charges": draw_bond_charges(jax.random.fold_in(jax.random.fold_in(arg_keys[6], part), 71), part),
    }


def live_rows(count, parity, position):
    limit = jnp.where(parity == 0, count, CHI - count)
    return (position < limit).astype(jnp.float32)


def reference(boundary, row_tensor, left_proj, right_proj, leg_parity, bond_charges):
    padded = 2 * BLOCK
    bound_all = boundary.reshape(COLS, padded, D, BLOCK)
    left_all = left_proj.reshape(COLS, padded, D, BLOCK)
    right_all = jnp.roll(right_proj.reshape(COLS, padded, D, BLOCK), -1, axis=0)
    charges_next = jnp.roll(bond_charges, -1, axis=0)
    legs_next = jnp.roll(leg_parity, -1, axis=0)
    indices = jnp.arange(padded, dtype=jnp.int32)
    parity_idx = indices // BLOCK
    position = indices % BLOCK
    inside = jnp.arange(BLOCK, dtype=jnp.int32)

    def column_step(inputs):
        bound_col, row_col, left_col, right_col, charge_here, charge_next, leg_here, leg_next = inputs
        left_leg = leg_here[0]
        up_leg = leg_here[1]
        down_leg = leg_here[2]
        right_leg = leg_next[0]
        bound_sel = (parity_idx[:, None] + up_leg[None, :]) % 2
        bound_mask = live_rows(charge_here[0], parity_idx, position)[:, None, None] * live_rows(
            charge_next[0], bound_sel[:, :, None], inside[None, None, :])
        bound_m = bound_col * bound_mask.astype(jnp.bfloat16)
        left_sel = (parity_idx[:, None] + left_leg[None, :]) % 2
        left_mask = live_rows(charge_here[1], parity_idx, position)[:, None, None] * live_rows(
            charge_here[0], left_sel[:, :, None], inside[None, None, :])
        left_m = left_col * left_mask.astype(jnp.bfloat16)
        left_dense = jnp.concatenate([
            left_m * (left_sel == 0).astype(jnp.bfloat16)[:, :, None],
            left_m * (left_sel == 1).astype(jnp.bfloat16)[:, :, None]], axis=2)
        right_sel = (parity_idx[:, None] + right_leg[None, :]) % 2
        right_mask = live_rows(charge_next[0], parity_idx, position)[:, None, None] * live_rows(
            charge_next[1], right_sel[:, :, None], inside[None, None, :])
        right_m = right_col * right_mask.astype(jnp.bfloat16)
        row_mask = ((left_leg[:, None, None, None] + up_leg[None, :, None, None]
                     + down_leg[None, None, :, None] + right_leg[None, None, None, :]) % 2 == 0).astype(jnp.float32)
        row_mask = row_mask * (1 - 2 * left_leg[:, None, None, None] * up_leg[None, :, None, None]).astype(jnp.float32)
        row_m = row_col * row_mask.astype(jnp.bfloat16)
        absorbed = jnp.dot(left_dense.reshape(padded * D, padded), bound_m.reshape(padded, D * BLOCK),
                           preferred_element_type=jnp.float32)
        absorbed = absorbed.astype(jnp.bfloat16).reshape(padded, D, D, BLOCK)
        mixed = jnp.einsum("plub,ludr->pdrb", absorbed.astype(jnp.float32), row_m.astype(jnp.float32))
        block_par = (parity_idx[:, None, None] + down_leg[None, :, None] + right_leg[None, None, :]) % 2
        sign_flip = (1 - 2 * block_par * down_leg[None, :, None]).astype(jnp.float32)
        mixed = (mixed * sign_flip[:, :, :, None]).astype(jnp.bfloat16)
        mixed_dense = jnp.concatenate([
            mixed * (block_par == 0).astype(jnp.bfloat16)[:, :, :, None],
            mixed * (block_par == 1).astype(jnp.bfloat16)[:, :, :, None]], axis=3)
        right_rb = jnp.transpose(right_m, (1, 0, 2)).reshape(D * padded, BLOCK)
        result = jnp.dot(mixed_dense.reshape(padded * D, D * padded), right_rb,
                         preferred_element_type=jnp.float32)
        return result.astype(jnp.bfloat16).reshape(padded, D * BLOCK)

    return lax.map(column_step, (bound_all, row_tensor, left_all, right_all,
                                 bond_charges, charges_next, leg_parity, legs_next))
```

```python
import functools

import jax
import jax.numpy as jnp
from jax import lax
from jax.experimental import pallas as pl
from jax.experimental.pallas import tpu as pltpu
from jax.sharding import PartitionSpec as P

CHI = 128
BLOCK = 96
D = 6
LANES = 128
SUB = 8
PAIRS = D * D
KRON = PAIRS * SUB
META = 4 * D + 4
SHIFTS = (2, 1, 3)

BF16 = jnp.bfloat16
F32 = jnp.float32


def passed_along(x, axis, by):
    length = lax.axis_size(axis)
    return lax.ppermute(x, axis, [(i, (i + by) % length) for i in range(length)])


def limit_of(count, parity):
    return jnp.where(parity == 0, count, CHI - count)


def scalars(meta_ref, col):
    def leg(kind, i):
        return meta_ref[col * META + kind * D + i]

    charge = [meta_ref[col * META + 4 * D + i] for i in range(4)]
    return leg, charge


def by_six(index, values):
    out = jnp.full(index.shape, values[0], jnp.int32)
    for i in range(1, D):
        out = jnp.where(index == i, values[i], out)
    return out


def prep_kernel(meta_ref, blk_ref, left_ref, row_ref, dense_ref, kron_ref):
    cols, sub_rows, _ = left_ref.shape
    parity = blk_ref[0] * sub_rows // BLOCK
    dense_ref[...] = jnp.zeros_like(dense_ref)
    spread = (
        lax.broadcasted_iota(jnp.int32, (KRON, PAIRS), 0) // SUB
        == lax.broadcasted_iota(jnp.int32, (KRON, PAIRS), 1)
    ).astype(F32).astype(BF16)
    diag = (
        lax.broadcasted_iota(jnp.int32, (KRON, KRON), 0) % SUB
        == lax.broadcasted_iota(jnp.int32, (KRON, KRON), 1) % SUB
    )
    pair_row = lax.broadcasted_iota(jnp.int32, (PAIRS, 1), 0)
    pair_col = lax.broadcasted_iota(jnp.int32, (1, PAIRS), 1)

    def one(col, carry):
        leg, _ = scalars(meta_ref, col)
        for l in range(D):
            piece = left_ref[col, :, l * BLOCK : (l + 1) * BLOCK]
            sel = (parity + leg(0, l)) % 2
            start = pl.multiple_of(sel * LANES, LANES)
            dense_ref[col, l * sub_rows : (l + 1) * sub_rows, pl.ds(start, LANES)] = jnp.concatenate(
                [piece, jnp.zeros((sub_rows, LANES - BLOCK), BF16)], axis=1
            )
        left_leg = by_six(pair_row // D, [leg(0, i) for i in range(D)])
        up_leg = by_six(pair_row % D, [leg(1, i) for i in range(D)])
        down_leg = by_six(pair_col // D, [leg(2, i) for i in range(D)])
        right_leg = by_six(pair_col % D, [leg(3, i) for i in range(D)])
        keep = (left_leg + up_leg + down_leg + right_leg) % 2 == 0
        block_par = (parity + down_leg + right_leg) % 2
        sign = (1 - 2 * left_leg * up_leg) * (1 - 2 * block_par * down_leg)
        row = row_ref[col].astype(F32) * jnp.where(keep, sign, 0).astype(F32)
        half = lax.dot_general(
            spread, row.astype(BF16), (((1,), (1,)), ((), ())), preferred_element_type=F32
        )
        full = lax.dot_general(
            half.astype(BF16), spread, (((1,), (1,)), ((), ())), preferred_element_type=F32
        )
        kron_ref[col] = jnp.where(diag, full, 0.0).astype(BF16)
        return carry

    lax.fori_loop(0, cols, one, 0)


def absorb_kernel(meta_ref, blk_ref, *refs):
    pieces, (dense_ref, kron_ref, mixed_ref, bound, total, split) = refs[:4], refs[4:]
    cols, sub_rows, _ = pieces[0].shape
    blk = blk_ref[0]
    groups = sub_rows // (2 * SUB)
    bound[...] = jnp.zeros_like(bound)
    row_at = lax.broadcasted_iota(jnp.int32, (sub_rows, BLOCK), 0)
    col_at = lax.broadcasted_iota(jnp.int32, (sub_rows, BLOCK), 1)

    def one(col, carry):
        leg, (in_here, _, in_next, _) = scalars(meta_ref, col)
        for piece, shift in zip(pieces, (0,) + SHIFTS):
            first = (blk + 4 - shift) % 4 * sub_rows
            parity = first // BLOCK
            place = first % BLOCK
            rows_live = row_at < limit_of(in_here, parity) - place
            start = pl.multiple_of(parity * LANES + place, 2 * SUB)
            for u in range(D):
                sel = (parity + leg(1, u)) % 2
                live = rows_live & (col_at < limit_of(in_next, sel))
                mask = jnp.where(live, 1.0, 0.0).astype(BF16)
                part = piece[col, :, u * BLOCK : (u + 1) * BLOCK] * mask
                bound[pl.ds(start, sub_rows), u * LANES : u * LANES + BLOCK] = part
        total[...] = jnp.dot(dense_ref[col], bound[...], preferred_element_type=F32)
        for l in range(D):
            for group in range(groups):
                for side in range(2):
                    at = l * sub_rows + (2 * group + side) * SUB
                    for u in range(0, D, 2):
                        both = jnp.concatenate(
                            [
                                total[at : at + SUB, u * LANES : (u + 1) * LANES],
                                total[at : at + SUB, (u + 1) * LANES : (u + 2) * LANES],
                            ],
                            axis=0,
                        )
                        to = (l * D + u) * SUB
                        split[group, to : to + 2 * SUB, side * LANES : (side + 1) * LANES] = both.astype(BF16)
        for group in range(groups):
            out = jnp.dot(kron_ref[col], split[group], preferred_element_type=F32)
            for d in range(D):
                for r in range(D):
                    at = (d * D + r) * SUB
                    both = jnp.concatenate(
                        [out[at : at + SUB, :LANES], out[at : at + SUB, LANES:]], axis=0
                    )
                    to = d * sub_rows + group * 2 * SUB
                    mixed_ref[col, to : to + 2 * SUB, r * LANES : (r + 1) * LANES] = both.astype(BF16)
        return carry

    lax.fori_loop(0, cols, one, 0)


def close_kernel(meta_ref, blk_ref, *refs):
    pieces, (mixed_ref, out_ref, right) = refs[:4], refs[4:]
    cols, sub_rows, _ = pieces[0].shape
    blk = blk_ref[0]
    own = blk * sub_rows
    own_parity = own // BLOCK
    own_place = own % BLOCK
    right[...] = jnp.zeros_like(right)
    row_at = lax.broadcasted_iota(jnp.int32, (sub_rows, BLOCK), 0)
    col_at = lax.broadcasted_iota(jnp.int32, (sub_rows, BLOCK), 1)

    def one(col, carry):
        leg, (_, out_here, _, out_next) = scalars(meta_ref, col)
        for piece, shift in zip(pieces, (0,) + SHIFTS):
            first = (blk + 4 - shift) % 4 * sub_rows
            parity = first // BLOCK
            place = first % BLOCK
            for r in range(D):
                sel = (parity + leg(3, r)) % 2
                start = pl.multiple_of(r * LANES + place, 2 * SUB)
                right[sel, pl.ds(start, sub_rows), :BLOCK] = piece[col, :, r * BLOCK : (r + 1) * BLOCK]
        both = jnp.concatenate([right[0], right[1]], axis=1)
        out = jnp.dot(mixed_ref[col], both, preferred_element_type=F32)
        rows_live = row_at < limit_of(out_here, own_parity) - own_place
        for d in range(D):
            sel = (own_parity + leg(2, d)) % 2
            rows = out[d * sub_rows : (d + 1) * sub_rows]
            picked = jnp.where(sel == 0, rows[:, :BLOCK], rows[:, LANES : LANES + BLOCK])
            live = rows_live & (col_at < limit_of(out_next, sel))
            out_ref[col, :, d * BLOCK : (d + 1) * BLOCK] = jnp.where(live, picked, 0.0).astype(BF16)
        return carry

    lax.fori_loop(0, cols, one, 0)


SMEM = pl.BlockSpec(memory_space=pltpu.SMEM)
VMEM = pl.BlockSpec(memory_space=pltpu.VMEM)


def per_device(boundary, row_tensor, left_proj, right_proj, leg_parity, bond_charges):
    cols, sub_rows, merged = boundary.shape
    bonds = leg_parity.shape[0]
    start_col = lax.axis_index("col") * cols
    after = lax.rem(start_col + cols, bonds)
    legs = jnp.concatenate(
        [
            lax.dynamic_slice_in_dim(leg_parity, start_col, cols, 0),
            lax.dynamic_slice_in_dim(leg_parity, after, 1, 0),
        ],
        axis=0,
    )
    charges = jnp.concatenate(
        [
            lax.dynamic_slice_in_dim(bond_charges, start_col, cols, 0),
            lax.dynamic_slice_in_dim(bond_charges, after, 1, 0),
        ],
        axis=0,
    )
    meta = jnp.concatenate(
        [legs[:cols].reshape(cols, 3 * D), legs[1:, 0], charges[:cols], charges[1:]], axis=1
    ).reshape(cols * META)
    blk = lax.axis_index("blk").astype(jnp.int32).reshape(1)

    bound_pieces = [boundary] + [passed_along(boundary, "blk", s) for s in SHIFTS]
    halo = passed_along(right_proj[:1], "col", -1)
    right_next = jnp.concatenate([right_proj[1:], halo], axis=0)
    right_pieces = [right_next] + [passed_along(right_next, "blk", s) for s in SHIFTS]

    dense, kron = pl.pallas_call(
        prep_kernel,
        out_shape=(
            jax.ShapeDtypeStruct((cols, D * sub_rows, 2 * LANES), BF16),
            jax.ShapeDtypeStruct((cols, KRON, KRON), BF16),
        ),
        in_specs=[SMEM, SMEM, VMEM, VMEM],
        out_specs=(VMEM, VMEM),
        cost_estimate=pl.CostEstimate(flops=10**8, bytes_accessed=10**6, transcendentals=0),
        name="prep",
    )(meta, blk, left_proj, row_tensor.reshape(cols, PAIRS, PAIRS))

    mixed = pl.pallas_call(
        absorb_kernel,
        out_shape=jax.ShapeDtypeStruct((cols, D * sub_rows, D * LANES), BF16),
        in_specs=[SMEM, SMEM] + [VMEM] * 6,
        out_specs=VMEM,
        scratch_shapes=[
            pltpu.VMEM((2 * LANES, D * LANES), BF16),
            pltpu.VMEM((D * sub_rows, D * LANES), F32),
            pltpu.VMEM((sub_rows // (2 * SUB), KRON, 2 * LANES), BF16),
        ],
        cost_estimate=pl.CostEstimate(flops=10**9, bytes_accessed=4 * 10**6, transcendentals=0),
        name="absorb",
    )(meta, blk, *bound_pieces, dense, kron)

    return pl.pallas_call(
        close_kernel,
        out_shape=jax.ShapeDtypeStruct((cols, sub_rows, merged), BF16),
        in_specs=[SMEM, SMEM] + [VMEM] * 5,
        out_specs=VMEM,
        scratch_shapes=[pltpu.VMEM((2, D * LANES, LANES), BF16)],
        cost_estimate=pl.CostEstimate(flops=10**9, bytes_accessed=3 * 10**6, transcendentals=0),
        name="close",
    )(meta, blk, *right_pieces, mixed)


def solution(mesh):
    in_specs = (
        P(("grp", "col"), "blk", None),
        P(("grp", "col"), None, None, None, None),
        P(("grp", "col"), "blk", None),
        P(("grp", "col"), "blk", None),
        P("grp", None, None),
        P("grp", None),
    )
    out_specs = P(("grp", "col"), "blk", None)
    return jax.shard_map(
        per_device, mesh=mesh, in_specs=in_specs, out_specs=out_specs, check_vma=False
    )
```

```python
import jax
import jax.numpy as jnp
from jax import lax
from jax.experimental import pallas as pl
from jax.experimental.pallas import tpu as pltpu
from jax.sharding import PartitionSpec as P


CHI = 128
BLOCK = 96
D = 6
LANES = 128
SUB = 8
PAIRS = D * D
KRON = PAIRS * SUB
SHIFTS = (2, 3, 1)
VMEM_LIMIT = 20 * 1024 * 1024

BF16 = jnp.bfloat16
F32 = jnp.float32


def passed_along(x, axis, by):
    length = lax.axis_size(axis)
    return lax.ppermute(x, axis, [(i, (i + by) % length) for i in range(length)])


def limit_of(count, parity):
    return jnp.where(parity == 0, count, CHI - count)


def by_six(index, values):
    out = jnp.full(index.shape, values[0], jnp.int32)
    for i in range(1, D):
        out = jnp.where(index == i, values[i], out)
    return out


def own_rows(sub_rows):
    first = lax.axis_index("blk") * sub_rows
    return first // BLOCK, first % BLOCK


def piece_rows(shift, sub_rows):
    count = lax.axis_size("blk")
    first = (lax.axis_index("blk") + count - shift) % count * sub_rows
    return first // BLOCK, first % BLOCK


class Tables:
    def __init__(self, legs_ref, charges_ref, legs, charges, sems):
        self.legs, self.charges = legs, charges
        self.copies = [
            pltpu.make_async_copy(legs_ref, legs, sems.at[0]),
            pltpu.make_async_copy(charges_ref, charges, sems.at[1]),
        ]
        self.bonds = legs.shape[2]

    def start(self):
        for copy in self.copies:
            copy.start()

    def wait(self):
        for copy in self.copies:
            copy.wait()

    def column(self, cols, col):
        here = lax.axis_index("col") * cols + col
        after = lax.rem(here + 1, self.bonds)
        legs = [[self.legs[kind, i, here] for i in range(D)] for kind in range(3)]
        legs.append([self.legs[0, i, after] for i in range(D)])
        charges = [self.charges[i, at] for at in (here, after) for i in range(2)]
        return legs, charges


def prep_kernel(
    legs_ref, charges_ref, left_ref, row_ref, dense_ref, kron_ref, live_ref, legs_s, charges_s, sems
):
    cols, sub_rows, _ = left_ref.shape
    tables = Tables(legs_ref, charges_ref, legs_s, charges_s, sems)
    tables.start()
    parity, _ = own_rows(sub_rows)
    dense_ref[...] = jnp.zeros_like(dense_ref)
    spread = (
        lax.broadcasted_iota(jnp.int32, (KRON, PAIRS), 0) // SUB
        == lax.broadcasted_iota(jnp.int32, (KRON, PAIRS), 1)
    ).astype(F32).astype(BF16)
    diag = (
        lax.broadcasted_iota(jnp.int32, (KRON, KRON), 0) % SUB
        == lax.broadcasted_iota(jnp.int32, (KRON, KRON), 1) % SUB
    )
    pair_row = lax.broadcasted_iota(jnp.int32, (PAIRS, 1), 0)
    pair_col = lax.broadcasted_iota(jnp.int32, (1, PAIRS), 1)
    lane = lax.broadcasted_iota(jnp.int32, (1, LANES), 1)
    tables.wait()

    for col in range(cols):
        legs, (in_here, _, in_next, _) = tables.column(cols, col)
        for l in range(D):
            sel = (parity + legs[0][l]) % 2
            start = pl.multiple_of(sel * LANES, LANES)
            live = jnp.where(lane < limit_of(in_here, sel), 1.0, 0.0).astype(BF16)
            piece = jnp.concatenate(
                [left_ref[col, :, l * BLOCK : (l + 1) * BLOCK], jnp.zeros((sub_rows, LANES - BLOCK), BF16)],
                axis=1,
            )
            dense_ref[col, l * sub_rows : (l + 1) * sub_rows, pl.ds(start, LANES)] = piece * live
            for u in range(0, D, 2):
                rows = [
                    jnp.broadcast_to(
                        jnp.where(lane < limit_of(in_next, (sel + legs[1][v]) % 2), 1.0, 0.0), (SUB, LANES)
                    )
                    for v in (u, u + 1)
                ]
                at = (l * D + u) * SUB
                live_ref[col, at : at + 2 * SUB] = jnp.concatenate(rows, axis=0).astype(BF16)
        left_leg = by_six(pair_row // D, legs[0])
        up_leg = by_six(pair_row % D, legs[1])
        down_leg = by_six(pair_col // D, legs[2])
        right_leg = by_six(pair_col % D, legs[3])
        keep = (left_leg + up_leg + down_leg + right_leg) % 2 == 0
        block_par = (parity + down_leg + right_leg) % 2
        sign = (1 - 2 * left_leg * up_leg) * (1 - 2 * block_par * down_leg)
        row = row_ref[col].astype(F32) * jnp.where(keep, sign, 0).astype(F32)
        half = lax.dot_general(
            spread, row.astype(BF16), (((1,), (1,)), ((), ())), preferred_element_type=F32
        )
        full = lax.dot_general(
            half.astype(BF16), spread, (((1,), (1,)), ((), ())), preferred_element_type=F32
        )
        kron_ref[col] = jnp.where(diag, full, 0.0).astype(BF16)


def absorb_kernel(*refs):
    pieces, (dense_ref, kron_ref, live_ref, mixed_ref, bound, split) = refs[:4], refs[4:]
    cols, sub_rows, _ = pieces[0].shape
    groups = sub_rows // (2 * SUB)
    gap = jnp.zeros((LANES - BLOCK, D * LANES), BF16)
    for col in range(cols):
        bound[col, BLOCK:LANES] = gap
        bound[col, LANES + BLOCK :] = gap
    pad = jnp.zeros((sub_rows, LANES - BLOCK), BF16)

    for col in range(cols):
        for piece, shift in zip(pieces, (0,) + SHIFTS):
            parity, place = piece_rows(shift, sub_rows)
            start = pl.multiple_of(parity * LANES + place, 2 * SUB)
            for u in range(D):
                part = jnp.concatenate([piece[col, :, u * BLOCK : (u + 1) * BLOCK], pad], axis=1)
                bound[col, pl.ds(start, sub_rows), u * LANES : (u + 1) * LANES] = part
        for u in range(0, D, 2):
            total = jnp.dot(
                dense_ref[col], bound[col, :, u * LANES : (u + 2) * LANES], preferred_element_type=F32
            )
            for l in range(D):
                to = (l * D + u) * SUB
                live = live_ref[col, to : to + 2 * SUB]
                for group in range(groups):
                    for side in range(2):
                        at = l * sub_rows + (2 * group + side) * SUB
                        rows = total[at : at + SUB]
                        both = jnp.concatenate([rows[:, :LANES], rows[:, LANES:]], axis=0).astype(BF16)
                        split[col, group, to : to + 2 * SUB, side * LANES : (side + 1) * LANES] = both * live
        for group in range(groups):
            out = jnp.dot(kron_ref[col], split[col, group], preferred_element_type=F32)
            for d in range(D):
                for r in range(D):
                    at = (d * D + r) * SUB
                    rows = out[at : at + SUB]
                    both = jnp.concatenate([rows[:, :LANES], rows[:, LANES:]], axis=0).astype(BF16)
                    to = d * sub_rows + group * 2 * SUB
                    mixed_ref[col, to : to + 2 * SUB, r * LANES : (r + 1) * LANES] = both


def close_kernel(legs_ref, charges_ref, *refs):
    pieces, (mixed_ref, out_ref, right, legs_s, charges_s, sems) = refs[:4], refs[4:]
    cols, sub_rows, _ = pieces[0].shape
    tables = Tables(legs_ref, charges_ref, legs_s, charges_s, sems)
    tables.start()
    own_parity, own_place = own_rows(sub_rows)
    gap = jnp.zeros((LANES - BLOCK, LANES), BF16)
    pad = jnp.zeros((sub_rows, LANES - BLOCK), BF16)
    row_at = lax.broadcasted_iota(jnp.int32, (sub_rows, BLOCK), 0)
    col_at = lax.broadcasted_iota(jnp.int32, (sub_rows, BLOCK), 1)
    for col in range(cols):
        for r in range(D):
            for q in range(2):
                right[col, q, r, BLOCK:] = gap
        for piece, shift in zip(pieces, (0,) + SHIFTS):
            parity, place = piece_rows(shift, sub_rows)
            start = pl.multiple_of(place, 2 * SUB)
            for r in range(D):
                part = jnp.concatenate([piece[col, :, r * BLOCK : (r + 1) * BLOCK], pad], axis=1)
                right[col, parity, r, pl.ds(start, sub_rows)] = part
    tables.wait()
    for col in range(cols):
        legs, (_, out_here, _, out_next) = tables.column(cols, col)
        out = None
        for r in range(0, D, 2):
            both = jnp.concatenate(
                [
                    jnp.concatenate([right[col, legs[3][v], v], right[col, 1 - legs[3][v], v]], axis=1)
                    for v in (r, r + 1)
                ],
                axis=0,
            )
            term = jnp.dot(mixed_ref[col, :, r * LANES : (r + 2) * LANES], both, preferred_element_type=F32)
            out = term if out is None else out + term
        rows_live = row_at < limit_of(out_here, own_parity) - own_place
        for d in range(D):
            sel = (own_parity + legs[2][d]) % 2
            rows = out[d * sub_rows : (d + 1) * sub_rows]
            picked = jnp.where(sel == 0, rows[:, :BLOCK], rows[:, LANES : LANES + BLOCK])
            live = rows_live & (col_at < limit_of(out_next, sel))
            out_ref[col, :, d * BLOCK : (d + 1) * BLOCK] = jnp.where(live, picked, 0.0).astype(BF16)


def token_kernel(token_ref):
    token_ref[...] = jnp.zeros_like(token_ref)


def head_kernel(token_ref, right_ref, head_ref):
    head_ref[...] = right_ref[:1]


def join_kernel(right_ref, halo_ref, next_ref):
    cols = right_ref.shape[0]
    next_ref[: cols - 1] = right_ref[1:]
    next_ref[cols - 1 :] = halo_ref[...]


VMEM = pl.BlockSpec(memory_space=pltpu.VMEM)


def local(kernel, out_shape, operands, scratch=(), flops=0, limit=VMEM_LIMIT, space=pltpu.VMEM):
    leaves = jax.tree.leaves(out_shape)
    moved = sum(x.size * x.dtype.itemsize for x in [*operands, *leaves])
    return pl.pallas_call(
        kernel,
        out_shape=out_shape,
        in_specs=[pl.BlockSpec(memory_space=space)] * len(operands),
        out_specs=jax.tree.map(lambda _: VMEM, out_shape),
        scratch_shapes=list(scratch),
        cost_estimate=pl.CostEstimate(flops=flops, bytes_accessed=moved, transcendentals=0),
        compiler_params=pltpu.CompilerParams(vmem_limit_bytes=limit),
    )(*operands)


def per_device(boundary, row_tensor, left_proj, right_proj, leg_parity, bond_charges):
    cols, sub_rows, merged = boundary.shape
    legs = leg_parity.transpose(1, 2, 0)
    charges = bond_charges.T
    shape = jax.ShapeDtypeStruct
    tables = [
        pltpu.SMEM(legs.shape, jnp.int32),
        pltpu.SMEM(charges.shape, jnp.int32),
        pltpu.SemaphoreType.DMA((2,)),
    ]
    small = 2 * 1024 * 1024

    token = local(token_kernel, shape((SUB, LANES), F32), [], flops=4 * 10**9, limit=small)
    head = local(head_kernel, shape((1, sub_rows, merged), BF16), [token, right_proj], flops=4 * 10**9, limit=small)
    halo = passed_along(head, "col", -1)
    bound_pieces = [boundary]
    for s in SHIFTS:
        bound_pieces.append(passed_along(boundary, "blk", s))
    right_next = local(join_kernel, shape(right_proj.shape, BF16), [right_proj, halo], flops=4 * 10**9, limit=small)
    right_pieces = [right_next]
    for s in SHIFTS:
        right_pieces.append(passed_along(right_next, "blk", s))

    dense, kron, live = local(
        prep_kernel,
        (
            shape((cols, D * sub_rows, 2 * LANES), BF16),
            shape((cols, KRON, KRON), BF16),
            shape((cols, KRON, LANES), BF16),
        ),
        [legs, charges, left_proj, row_tensor.reshape(cols, PAIRS, PAIRS)],
        tables,
        flops=10**8,
    )
    mixed = local(
        absorb_kernel,
        shape((cols, D * sub_rows, D * LANES), BF16),
        [*bound_pieces, dense, kron, live],
        [
            pltpu.VMEM((cols, 2 * LANES, D * LANES), BF16),
            pltpu.VMEM((cols, sub_rows // (2 * SUB), KRON, 2 * LANES), BF16),
        ],
        flops=10**9,
    )
    return local(
        close_kernel,
        shape((cols, sub_rows, merged), BF16),
        [legs, charges, *right_pieces, mixed],
        [pltpu.VMEM((cols, 2, D, LANES, LANES), BF16), *tables],
        flops=10**9,
    )


def solution(mesh):
    in_specs = (
        P(("grp", "col"), "blk", None),
        P(("grp", "col"), None, None, None, None),
        P(("grp", "col"), "blk", None),
        P(("grp", "col"), "blk", None),
        P("grp", None, None),
        P("grp", None),
    )
    out_specs = P(("grp", "col"), "blk", None)
    return jax.shard_map(per_device, mesh=mesh, in_specs=in_specs, out_specs=out_specs, check_vma=False)
```

```python
import jax
import jax.numpy as jnp
from jax import lax
from jax.experimental import pallas as pl
from jax.experimental.pallas import tpu as pltpu
from jax.sharding import PartitionSpec as P


CHI = 128
BLOCK = 96
D = 6
LANES = 128
SUB = 8
PAIRS = D * D
KRON = PAIRS * SUB
SHIFTS = (2, 3, 1)
VMEM_LIMIT = 20 * 1024 * 1024

BF16 = jnp.bfloat16
F32 = jnp.float32


def passed_along(x, axis, by):
    length = lax.axis_size(axis)
    return lax.ppermute(x, axis, [(i, (i + by) % length) for i in range(length)])


def sent(x, by):
    return passed_along(x, "blk", by)


def limit_of(count, parity):
    return jnp.where(parity == 0, count, CHI - count)


def by_six(index, values):
    out = jnp.full(index.shape, values[0], jnp.int32)
    for i in range(1, D):
        out = jnp.where(index == i, values[i], out)
    return out


def own_rows(sub_rows):
    first = lax.axis_index("blk") * sub_rows
    return first // BLOCK, first % BLOCK


def piece_rows(shift, sub_rows):
    count = lax.axis_size("blk")
    first = (lax.axis_index("blk") + count - shift) % count * sub_rows
    return first // BLOCK, first % BLOCK


class Tables:
    def __init__(self, legs_ref, charges_ref, legs, charges, sems):
        self.legs, self.charges = legs, charges
        self.copies = [
            pltpu.make_async_copy(legs_ref, legs, sems.at[0]),
            pltpu.make_async_copy(charges_ref, charges, sems.at[1]),
        ]
        self.bonds = legs.shape[2]

    def start(self):
        for copy in self.copies:
            copy.start()

    def wait(self):
        for copy in self.copies:
            copy.wait()

    def column(self, cols, col):
        here = lax.axis_index("col") * cols + col
        after = lax.rem(here + 1, self.bonds)
        legs = [[self.legs[kind, i, here] for i in range(D)] for kind in range(3)]
        legs.append([self.legs[0, i, after] for i in range(D)])
        charges = [self.charges[i, at] for at in (here, after) for i in range(2)]
        return legs, charges


def prep_kernel(
    legs_ref, charges_ref, left_ref, row_ref, dense_ref, kron_ref, live_ref, legs_s, charges_s, sems
):
    cols, sub_rows, _ = left_ref.shape
    tables = Tables(legs_ref, charges_ref, legs_s, charges_s, sems)
    tables.start()
    parity, _ = own_rows(sub_rows)
    dense_ref[...] = jnp.zeros_like(dense_ref)
    spread = (
        lax.broadcasted_iota(jnp.int32, (KRON, PAIRS), 0) // SUB
        == lax.broadcasted_iota(jnp.int32, (KRON, PAIRS), 1)
    ).astype(F32).astype(BF16)
    diag = (
        lax.broadcasted_iota(jnp.int32, (KRON, KRON), 0) % SUB
        == lax.broadcasted_iota(jnp.int32, (KRON, KRON), 1) % SUB
    )
    pair_row = lax.broadcasted_iota(jnp.int32, (PAIRS, 1), 0)
    pair_col = lax.broadcasted_iota(jnp.int32, (1, PAIRS), 1)
    lane = lax.broadcasted_iota(jnp.int32, (1, LANES), 1)
    tables.wait()

    for col in range(cols):
        legs, (in_here, _, in_next, _) = tables.column(cols, col)
        for l in range(D):
            sel = (parity + legs[0][l]) % 2
            start = pl.multiple_of(sel * LANES, LANES)
            live = jnp.where(lane < limit_of(in_here, sel), 1.0, 0.0).astype(BF16)
            piece = jnp.concatenate(
                [left_ref[col, :, l * BLOCK : (l + 1) * BLOCK], jnp.zeros((sub_rows, LANES - BLOCK), BF16)],
                axis=1,
            )
            dense_ref[col, l * sub_rows : (l + 1) * sub_rows, pl.ds(start, LANES)] = piece * live
            for u in range(0, D, 2):
                rows = [
                    jnp.broadcast_to(
                        jnp.where(lane < limit_of(in_next, (sel + legs[1][v]) % 2), 1.0, 0.0), (SUB, LANES)
                    )
                    for v in (u, u + 1)
                ]
                at = (l * D + u) * SUB
                live_ref[col, at : at + 2 * SUB] = jnp.concatenate(rows, axis=0).astype(BF16)
        left_leg = by_six(pair_row // D, legs[0])
        up_leg = by_six(pair_row % D, legs[1])
        down_leg = by_six(pair_col // D, legs[2])
        right_leg = by_six(pair_col % D, legs[3])
        keep = (left_leg + up_leg + down_leg + right_leg) % 2 == 0
        block_par = (parity + down_leg + right_leg) % 2
        sign = (1 - 2 * left_leg * up_leg) * (1 - 2 * block_par * down_leg)
        row = row_ref[col].astype(F32) * jnp.where(keep, sign, 0).astype(F32)
        half = lax.dot_general(
            spread, row.astype(BF16), (((1,), (1,)), ((), ())), preferred_element_type=F32
        )
        full = lax.dot_general(
            half.astype(BF16), spread, (((1,), (1,)), ((), ())), preferred_element_type=F32
        )
        kron_ref[col] = jnp.where(diag, full, 0.0).astype(BF16)


def absorb_kernel(*refs):
    pieces, (dense_ref, kron_ref, live_ref, mixed_ref, bound, split) = refs[:4], refs[4:]
    cols, sub_rows, _ = pieces[0].shape
    groups = sub_rows // (2 * SUB)
    gap = jnp.zeros((LANES - BLOCK, D * LANES), BF16)
    for col in range(cols):
        bound[col, BLOCK:LANES] = gap
        bound[col, LANES + BLOCK :] = gap
    pad = jnp.zeros((sub_rows, LANES - BLOCK), BF16)

    for col in range(cols):
        for piece, shift in zip(pieces, (0,) + SHIFTS):
            parity, place = piece_rows(shift, sub_rows)
            start = pl.multiple_of(parity * LANES + place, 2 * SUB)
            for u in range(D):
                part = jnp.concatenate([piece[col, :, u * BLOCK : (u + 1) * BLOCK], pad], axis=1)
                bound[col, pl.ds(start, sub_rows), u * LANES : (u + 1) * LANES] = part
        for u in range(0, D, 2):
            total = jnp.dot(
                dense_ref[col], bound[col, :, u * LANES : (u + 2) * LANES], preferred_element_type=F32
            )
            for l in range(D):
                to = (l * D + u) * SUB
                live = live_ref[col, to : to + 2 * SUB]
                for group in range(groups):
                    for side in range(2):
                        at = l * sub_rows + (2 * group + side) * SUB
                        rows = total[at : at + SUB]
                        both = jnp.concatenate([rows[:, :LANES], rows[:, LANES:]], axis=0).astype(BF16)
                        split[col, group, to : to + 2 * SUB, side * LANES : (side + 1) * LANES] = both * live
        for group in range(groups):
            out = jnp.dot(kron_ref[col], split[col, group], preferred_element_type=F32)
            for d in range(D):
                for r in range(D):
                    at = (d * D + r) * SUB
                    rows = out[at : at + SUB]
                    both = jnp.concatenate([rows[:, :LANES], rows[:, LANES:]], axis=0).astype(BF16)
                    to = d * sub_rows + group * 2 * SUB
                    mixed_ref[col, to : to + 2 * SUB, r * LANES : (r + 1) * LANES] = both


def close_kernel(legs_ref, charges_ref, *refs):
    own, far, far_last, *near = refs[:5]
    mixed_ref, out_ref, right, legs_s, charges_s, sems = refs[5:]
    cols, sub_rows, _ = own.shape
    tables = Tables(legs_ref, charges_ref, legs_s, charges_s, sems)
    tables.start()
    own_parity, own_place = own_rows(sub_rows)
    gap = jnp.zeros((LANES - BLOCK, LANES), BF16)
    pad = jnp.zeros((sub_rows, LANES - BLOCK), BF16)
    row_at = lax.broadcasted_iota(jnp.int32, (sub_rows, BLOCK), 0)
    col_at = lax.broadcasted_iota(jnp.int32, (sub_rows, BLOCK), 1)
    for col in range(cols):
        for r in range(D):
            for q in range(2):
                right[col, q, r, BLOCK:] = gap
        second = (far, col) if col < cols - 1 else (far_last, 0)
        pieces = [(own, col), second, *((piece, col) for piece in near)]
        for (piece, at), shift in zip(pieces, (0,) + SHIFTS):
            parity, place = piece_rows(shift, sub_rows)
            start = pl.multiple_of(place, 2 * SUB)
            for r in range(D):
                part = jnp.concatenate([piece[at, :, r * BLOCK : (r + 1) * BLOCK], pad], axis=1)
                right[col, parity, r, pl.ds(start, sub_rows)] = part
    tables.wait()
    for col in range(cols):
        legs, (_, out_here, _, out_next) = tables.column(cols, col)
        out = None
        for r in range(0, D, 2):
            both = jnp.concatenate(
                [
                    jnp.concatenate([right[col, legs[3][v], v], right[col, 1 - legs[3][v], v]], axis=1)
                    for v in (r, r + 1)
                ],
                axis=0,
            )
            term = jnp.dot(mixed_ref[col, :, r * LANES : (r + 2) * LANES], both, preferred_element_type=F32)
            out = term if out is None else out + term
        rows_live = row_at < limit_of(out_here, own_parity) - own_place
        for d in range(D):
            sel = (own_parity + legs[2][d]) % 2
            rows = out[d * sub_rows : (d + 1) * sub_rows]
            picked = jnp.where(sel == 0, rows[:, :BLOCK], rows[:, LANES : LANES + BLOCK])
            live = rows_live & (col_at < limit_of(out_next, sel))
            out_ref[col, :, d * BLOCK : (d + 1) * BLOCK] = jnp.where(live, picked, 0.0).astype(BF16)


def token_kernel(token_ref):
    token_ref[...] = jnp.zeros_like(token_ref)


def split_kernel(token_ref, right_ref, head_ref, tail_ref):
    head_ref[...] = right_ref[:1]
    tail_ref[...] = right_ref[1:]


def join_kernel(right_ref, halo_ref, next_ref):
    cols = right_ref.shape[0]
    next_ref[: cols - 1] = right_ref[1:]
    next_ref[cols - 1 :] = halo_ref[...]


VMEM = pl.BlockSpec(memory_space=pltpu.VMEM)


def local(kernel, out_shape, operands, scratch=(), flops=0, limit=VMEM_LIMIT, space=pltpu.VMEM):
    leaves = jax.tree.leaves(out_shape)
    moved = sum(x.size * x.dtype.itemsize for x in [*operands, *leaves])
    return pl.pallas_call(
        kernel,
        out_shape=out_shape,
        in_specs=[pl.BlockSpec(memory_space=space)] * len(operands),
        out_specs=jax.tree.map(lambda _: VMEM, out_shape),
        scratch_shapes=list(scratch),
        cost_estimate=pl.CostEstimate(flops=flops, bytes_accessed=moved, transcendentals=0),
        compiler_params=pltpu.CompilerParams(vmem_limit_bytes=limit),
    )(*operands)


def per_device(boundary, row_tensor, left_proj, right_proj, leg_parity, bond_charges):
    cols, sub_rows, merged = boundary.shape
    legs = leg_parity.transpose(1, 2, 0)
    charges = bond_charges.T
    shape = jax.ShapeDtypeStruct
    tables = [
        pltpu.SMEM(legs.shape, jnp.int32),
        pltpu.SMEM(charges.shape, jnp.int32),
        pltpu.SemaphoreType.DMA((2,)),
    ]
    small = 2 * 1024 * 1024

    token = local(token_kernel, shape((SUB, LANES), F32), [], flops=4 * 10**9, limit=small)
    head, tail = local(
        split_kernel,
        (shape((1, sub_rows, merged), BF16), shape((cols - 1, sub_rows, merged), BF16)),
        [token, right_proj],
        flops=4 * 10**9,
        limit=small,
    )
    halo = passed_along(head, "col", -1)
    bound_pieces = [boundary] + [sent(boundary, s) for s in SHIFTS]
    right_next = local(join_kernel, shape(right_proj.shape, BF16), [right_proj, halo], flops=4 * 10**9, limit=small)
    far, *near = SHIFTS
    right_pieces = [right_next, sent(tail, far), sent(halo, far)]
    right_pieces += [sent(right_next, s) for s in near]

    dense, kron, live = local(
        prep_kernel,
        (
            shape((cols, D * sub_rows, 2 * LANES), BF16),
            shape((cols, KRON, KRON), BF16),
            shape((cols, KRON, LANES), BF16),
        ),
        [legs, charges, left_proj, row_tensor.reshape(cols, PAIRS, PAIRS)],
        tables,
        flops=10**8,
    )
    mixed = local(
        absorb_kernel,
        shape((cols, D * sub_rows, D * LANES), BF16),
        [*bound_pieces, dense, kron, live],
        [
            pltpu.VMEM((cols, 2 * LANES, D * LANES), BF16),
            pltpu.VMEM((cols, sub_rows // (2 * SUB), KRON, 2 * LANES), BF16),
        ],
        flops=10**9,
    )
    return local(
        close_kernel,
        shape((cols, sub_rows, merged), BF16),
        [legs, charges, *right_pieces, mixed],
        [pltpu.VMEM((cols, 2, D, LANES, LANES), BF16), *tables],
        flops=10**9,
    )


def solution(mesh):
    in_specs = (
        P(("grp", "col"), "blk", None),
        P(("grp", "col"), None, None, None, None),
        P(("grp", "col"), "blk", None),
        P(("grp", "col"), "blk", None),
        P("grp", None, None),
        P("grp", None),
    )
    out_specs = P(("grp", "col"), "blk", None)
    return jax.shard_map(per_device, mesh=mesh, in_specs=in_specs, out_specs=out_specs, check_vma=False)
```

```python
import jax
import jax.numpy as jnp
from jax import lax
from jax.experimental import pallas as pl
from jax.experimental.pallas import tpu as pltpu
from jax.sharding import PartitionSpec as P


CHI = 128
BLOCK = 96
D = 6
LANES = 128
SUB = 8
PAIRS = D * D
KRON = PAIRS * SUB
WIDTH = 6
SHIFTS = (2, 3, 1)
RIGHT_SHIFTS = (2, 1, 3)
VMEM_LIMIT = 20 * 1024 * 1024

BF16 = jnp.bfloat16
F32 = jnp.float32


def passed_along(x, axis, by):
    length = lax.axis_size(axis)
    return lax.ppermute(x, axis, [(i, (i + by) % length) for i in range(length)])


def sent(x, by):
    return passed_along(x, "blk", by)


def limit_of(count, parity):
    return jnp.where(parity == 0, count, CHI - count)


def by_six(index, values):
    out = jnp.zeros(index.shape, jnp.int32)
    for i in range(D):
        out = jnp.where(index == i, values[i], out)
    return out


def own_rows(sub_rows):
    first = lax.axis_index("blk") * sub_rows
    return first // BLOCK, first % BLOCK


def piece_rows(shift, sub_rows):
    count = lax.axis_size("blk")
    first = (lax.axis_index("blk") + count - shift) % count * sub_rows
    return first // BLOCK, first % BLOCK


class Table:
    def __init__(self, table_ref, table, sem):
        self.table = table
        self.copy = pltpu.make_async_copy(table_ref, table, sem)

    def column(self, col):
        def at(slot, step):
            return self.table[0, slot * WIDTH + col + step]

        legs = [[at(kind * D + i, 0) for i in range(D)] for kind in range(3)]
        legs.append([at(i, 1) for i in range(D)])
        charges = [at(3 * D + i, step) for step in range(2) for i in range(2)]
        return legs, charges


def packed_table(legs_ref, charges_ref, cols):
    bonds = legs_ref.shape[2]
    here = lax.axis_index("col") * cols
    lane = lax.broadcasted_iota(jnp.int32, (1, bonds), 1)
    rows = [legs_ref[kind, i : i + 1] for kind in range(3) for i in range(D)]
    rows += [charges_ref[i : i + 1] for i in range(2)]
    table = jnp.zeros((1, bonds), jnp.int32)
    for slot, row in enumerate(rows):
        turned = pltpu.roll(row, lax.rem(bonds - here + slot * WIDTH, bonds), 1)
        table = jnp.where(lane // WIDTH == slot, turned, table)
    return table


def prep_kernel(table_ref, left_ref, row_ref, dense_ref, kron_ref, live_ref):
    cols, sub_rows, _ = left_ref.shape
    parity, _ = own_rows(sub_rows)
    table = table_ref[...]
    spread = (
        lax.broadcasted_iota(jnp.int32, (KRON, PAIRS), 0) // SUB
        == lax.broadcasted_iota(jnp.int32, (KRON, PAIRS), 1)
    ).astype(F32).astype(BF16)
    diag = (
        lax.broadcasted_iota(jnp.int32, (KRON, KRON), 0) % SUB
        == lax.broadcasted_iota(jnp.int32, (KRON, KRON), 1) % SUB
    )
    pair_row = lax.broadcasted_iota(jnp.int32, (PAIRS, 1), 0)
    pair_col = lax.broadcasted_iota(jnp.int32, (1, PAIRS), 1)
    lane = lax.broadcasted_iota(jnp.int32, (1, LANES), 1)
    pad = jnp.zeros((sub_rows, LANES - BLOCK), BF16)

    def at(slot, step):
        return table[:, slot * WIDTH + step : slot * WIDTH + step + 1]

    def below(limit):
        return jnp.where(lane < limit, 1, 0)

    for col in range(cols):
        left_leg = [at(i, col) for i in range(D)]
        up_leg = [at(D + i, col) for i in range(D)]
        down_leg = [at(2 * D + i, col) for i in range(D)]
        right_leg = [at(i, col + 1) for i in range(D)]
        in_here = at(3 * D, col)
        in_next = at(3 * D, col + 1)
        here = [below(in_here), below(CHI - in_here)]
        after = [below(in_next), below(CHI - in_next)]
        for l in range(D):
            sel = (parity + left_leg[l]) % 2
            piece = jnp.concatenate([left_ref[col, :, l * BLOCK : (l + 1) * BLOCK], pad], axis=1)
            for half in range(2):
                live = (here[half] * (sel if half else 1 - sel)).astype(F32).astype(BF16)
                dense_ref[col, l * sub_rows : (l + 1) * sub_rows, half * LANES : (half + 1) * LANES] = piece * live
            for u in range(0, D, 2):
                rows = []
                for v in (u, u + 1):
                    odd = (sel + up_leg[v]) % 2
                    row = after[0] * (1 - odd) + after[1] * odd
                    rows.append(jnp.broadcast_to(row.astype(F32), (SUB, LANES)))
                to = (l * D + u) * SUB
                live_ref[col, to : to + 2 * SUB] = jnp.concatenate(rows, axis=0).astype(BF16)
        left_at = by_six(pair_row // D, left_leg)
        up_at = by_six(pair_row % D, up_leg)
        down_at = by_six(pair_col // D, down_leg)
        right_at = by_six(pair_col % D, right_leg)
        keep = (left_at + up_at + down_at + right_at) % 2 == 0
        block_par = (parity + down_at + right_at) % 2
        sign = (1 - 2 * left_at * up_at) * (1 - 2 * block_par * down_at)
        row = row_ref[col].astype(F32) * jnp.where(keep, sign, 0).astype(F32)
        half = lax.dot_general(
            spread, row.astype(BF16), (((1,), (1,)), ((), ())), preferred_element_type=F32
        )
        full = lax.dot_general(
            half.astype(BF16), spread, (((1,), (1,)), ((), ())), preferred_element_type=F32
        )
        kron_ref[col] = jnp.where(diag, full, 0.0).astype(BF16)


def absorb_kernel(*refs):
    pieces, (dense_ref, kron_ref, live_ref, mixed_ref, bound, split) = refs[:4], refs[4:]
    cols, sub_rows, _ = pieces[0].shape
    groups = sub_rows // (2 * SUB)
    gap = jnp.zeros((LANES - BLOCK, D * LANES), BF16)
    for col in range(cols):
        bound[col, BLOCK:LANES] = gap
        bound[col, LANES + BLOCK :] = gap
    pad = jnp.zeros((sub_rows, LANES - BLOCK), BF16)

    for col in range(cols):
        for piece, shift in zip(pieces, (0,) + SHIFTS):
            parity, place = piece_rows(shift, sub_rows)
            start = pl.multiple_of(parity * LANES + place, 2 * SUB)
            for u in range(D):
                part = jnp.concatenate([piece[col, :, u * BLOCK : (u + 1) * BLOCK], pad], axis=1)
                bound[col, pl.ds(start, sub_rows), u * LANES : (u + 1) * LANES] = part
        for u in range(0, D, 2):
            total = jnp.dot(
                dense_ref[col], bound[col, :, u * LANES : (u + 2) * LANES], preferred_element_type=F32
            )
            for l in range(D):
                to = (l * D + u) * SUB
                live = live_ref[col, to : to + 2 * SUB]
                for group in range(groups):
                    for side in range(2):
                        at = l * sub_rows + (2 * group + side) * SUB
                        rows = total[at : at + SUB]
                        both = jnp.concatenate([rows[:, :LANES], rows[:, LANES:]], axis=0).astype(BF16)
                        split[col, group, to : to + 2 * SUB, side * LANES : (side + 1) * LANES] = both * live
        for group in range(groups):
            out = jnp.dot(kron_ref[col], split[col, group], preferred_element_type=F32)
            for d in range(D):
                for r in range(D):
                    at = (d * D + r) * SUB
                    rows = out[at : at + SUB]
                    both = jnp.concatenate([rows[:, :LANES], rows[:, LANES:]], axis=0).astype(BF16)
                    to = d * sub_rows + group * 2 * SUB
                    mixed_ref[col, to : to + 2 * SUB, r * LANES : (r + 1) * LANES] = both


def close_kernel(table_ref, *refs):
    own, tails, lasts, across = refs[0], refs[1:3], refs[3:5], refs[5]
    mixed_ref, out_ref, right, table_s, sem = refs[6:]
    cols, sub_rows, _ = own.shape
    table = Table(table_ref, table_s, sem)
    table.copy.start()
    own_parity, own_place = own_rows(sub_rows)
    gap = jnp.zeros((LANES - BLOCK, LANES), BF16)
    pad = jnp.zeros((sub_rows, LANES - BLOCK), BF16)
    row_at = lax.broadcasted_iota(jnp.int32, (sub_rows, BLOCK), 0)
    col_at = lax.broadcasted_iota(jnp.int32, (sub_rows, BLOCK), 1)
    for col in range(cols):
        for r in range(D):
            for q in range(2):
                right[col, q, r, BLOCK:] = gap
        near = [(piece, col) for piece in tails] if col < cols - 1 else [(piece, 0) for piece in lasts]
        pieces = [(own, col), *near, (across, col)]
        for (piece, at), shift in zip(pieces, (0,) + RIGHT_SHIFTS):
            parity, place = piece_rows(shift, sub_rows)
            start = pl.multiple_of(place, 2 * SUB)
            for r in range(D):
                part = jnp.concatenate([piece[at, :, r * BLOCK : (r + 1) * BLOCK], pad], axis=1)
                right[col, parity, r, pl.ds(start, sub_rows)] = part
    table.copy.wait()
    for col in range(cols):
        legs, (_, out_here, _, out_next) = table.column(col)
        out = None
        for r in range(0, D, 2):
            both = jnp.concatenate(
                [
                    jnp.concatenate([right[col, legs[3][v], v], right[col, 1 - legs[3][v], v]], axis=1)
                    for v in (r, r + 1)
                ],
                axis=0,
            )
            term = jnp.dot(mixed_ref[col, :, r * LANES : (r + 2) * LANES], both, preferred_element_type=F32)
            out = term if out is None else out + term
        rows_live = row_at < limit_of(out_here, own_parity) - own_place
        for d in range(D):
            sel = (own_parity + legs[2][d]) % 2
            rows = out[d * sub_rows : (d + 1) * sub_rows]
            picked = jnp.where(sel == 0, rows[:, :BLOCK], rows[:, LANES : LANES + BLOCK])
            live = rows_live & (col_at < limit_of(out_next, sel))
            out_ref[col, :, d * BLOCK : (d + 1) * BLOCK] = jnp.where(live, picked, 0.0).astype(BF16)


def token_kernel(token_ref):
    token_ref[...] = jnp.zeros_like(token_ref)


def split_kernel(token_ref, right_ref, head_ref, tail_ref):
    head_ref[...] = right_ref[:1]
    tail_ref[...] = right_ref[1:]


def join_kernel(right_ref, halo_ref, legs_ref, charges_ref, next_ref, table_ref):
    cols = right_ref.shape[0]
    table_ref[...] = packed_table(legs_ref, charges_ref, cols)
    next_ref[: cols - 1] = right_ref[1:]
    next_ref[cols - 1 :] = halo_ref[...]


VMEM = pl.BlockSpec(memory_space=pltpu.VMEM)


def local(kernel, out_shape, operands, scratch=(), flops=0, limit=VMEM_LIMIT, space=pltpu.VMEM):
    leaves = jax.tree.leaves(out_shape)
    moved = sum(x.size * x.dtype.itemsize for x in [*operands, *leaves])
    return pl.pallas_call(
        kernel,
        out_shape=out_shape,
        in_specs=[pl.BlockSpec(memory_space=space)] * len(operands),
        out_specs=jax.tree.map(lambda _: VMEM, out_shape),
        scratch_shapes=list(scratch),
        cost_estimate=pl.CostEstimate(flops=flops, bytes_accessed=moved, transcendentals=0),
        compiler_params=pltpu.CompilerParams(vmem_limit_bytes=limit),
    )(*operands)


def per_device(boundary, row_tensor, left_proj, right_proj, leg_parity, bond_charges):
    cols, sub_rows, merged = boundary.shape
    legs = leg_parity.transpose(1, 2, 0)
    charges = bond_charges.T
    shape = jax.ShapeDtypeStruct
    line = (1, legs.shape[2])
    lookup = [pltpu.SMEM(line, jnp.int32), pltpu.SemaphoreType.DMA]
    small = 2 * 1024 * 1024

    token = local(token_kernel, shape((SUB, LANES), F32), [], flops=4 * 10**9, limit=small)
    head, tail = local(
        split_kernel,
        (shape((1, sub_rows, merged), BF16), shape((cols - 1, sub_rows, merged), BF16)),
        [token, right_proj],
        flops=4 * 10**9,
        limit=small,
    )
    halo = passed_along(head, "col", -1)
    bound_pieces = [boundary] + [sent(boundary, s) for s in SHIFTS]
    right_next, table = local(
        join_kernel,
        (shape(right_proj.shape, BF16), shape(line, jnp.int32)),
        [right_proj, halo, legs, charges],
        flops=4 * 10**9,
        limit=small,
    )
    *near, far = RIGHT_SHIFTS
    tails = [sent(tail, s) for s in near]
    across = sent(right_next, far)
    lasts = [sent(halo, s) for s in near]
    right_pieces = [right_next, *tails, *lasts, across]

    dense, kron, live = local(
        prep_kernel,
        (
            shape((cols, D * sub_rows, 2 * LANES), BF16),
            shape((cols, KRON, KRON), BF16),
            shape((cols, KRON, LANES), BF16),
        ),
        [table, left_proj, row_tensor.reshape(cols, PAIRS, PAIRS)],
        flops=10**8,
    )
    mixed = local(
        absorb_kernel,
        shape((cols, D * sub_rows, D * LANES), BF16),
        [*bound_pieces, dense, kron, live],
        [
            pltpu.VMEM((cols, 2 * LANES, D * LANES), BF16),
            pltpu.VMEM((cols, sub_rows // (2 * SUB), KRON, 2 * LANES), BF16),
        ],
        flops=10**9,
    )
    return local(
        close_kernel,
        shape((cols, sub_rows, merged), BF16),
        [table, *right_pieces, mixed],
        [pltpu.VMEM((cols, 2, D, LANES, LANES), BF16), *lookup],
        flops=10**9,
    )


def solution(mesh):
    in_specs = (
        P(("grp", "col"), "blk", None),
        P(("grp", "col"), None, None, None, None),
        P(("grp", "col"), "blk", None),
        P(("grp", "col"), "blk", None),
        P("grp", None, None),
        P("grp", None),
    )
    out_specs = P(("grp", "col"), "blk", None)
    return jax.shard_map(per_device, mesh=mesh, in_specs=in_specs, out_specs=out_specs, check_vma=False)
```
